32 devices in a mesh: gx: 4 (over y, core), gy: 8 (over z, x).
Axes of the slice: x: 2, y: 2, z: 4, core: 2. Of those that a mesh axis runs over, the one named last changes fastest.
Arguments:
- pool_old: float32 [40, 131072], P(None, ('gx', 'gy')), may hold values from 0.5 to 2
- pool_new: float32 [40, 131072], P(None, ('gx', 'gy')), may hold values from 0.5 to 2
- flux: float32 [40, 131072], P(None, ('gx', 'gy')), may hold values from -6 to 6
- area: float32 [131072], P(('gx', 'gy')), may hold values from 0.05 to 1
- pft_id: int32 [131072], P(('gx', 'gy')), may hold values from 0 to 78
- region_id: int32 [131072], P(('gx', 'gy')), may hold values from 0 to 31, as said below
Outputs:
- pool_totals: float32 [40, 2528], replicated
- error_totals: float32 [40, 2528], replicated
The draws below stay inside these ranges and needn't reach their ends.
Inputs may be any that keep to these rules, and one draw needn't show every extreme that they name: `region_id`: patch i lies in block k = i // 4096; with K = 32 blocks, its region is (k * 32) // K or ((k * 32) // K + 1) mod 32.
All inputs are finite; a program needn't handle non-finite values.
Results may differ from the reference program's by a relative error of at most 0.000076.
Values sent between devices are 32-bit elements; how exact they have to be, the bound alone decides.
No kernel may reach another device: no remote copies, remote signals or barrier semaphores. Data moves between devices by JAX's collectives and lax.ppermute only.
A program may use at most 64 MiB of HBM per device.

```python
import math
import jax
import jax.numpy as jnp
import numpy as np

POOLS = 40
PFT = 79
REGION = 32
PATCH_DEV = 4096
CELLS = 2528
PATCHES = 131072
DEVICES = 32


def draw_region_id(key, part):
    index = jnp.arange(PATCHES, dtype=jnp.int32)
    block = index // PATCH_DEV
    base = block * REGION // DEVICES
    picks = jax.random.randint(key, (PATCHES,), 0, 4)
    region = jnp.where(picks == 0, base + 1, base) % REGION
    return region.astype(jnp.int32)


def plant(values, key, low, high):
    spot = [jax.random.randint(jax.random.fold_in(key, axis), (), 0, length) for axis, length in enumerate(values.shape)]
    widest = values.shape.index(max(values.shape))
    neighbour = spot[:widest] + [(spot[widest] + 1) % values.shape[widest]] + spot[widest + 1:]
    return values.at[tuple(spot)].set(low).at[tuple(neighbour)].set(high)


def block_levels(rng, extent, split, least, top_value):
    loudness, own = 1.0, jax.random.fold_in(rng, 6)
    for axis_at, blocks in split:
        steps = jnp.exp(jax.random.uniform(jax.random.fold_in(own, axis_at), (blocks,), jnp.float32, least / len(split), top_value / len(split)))
        loudness = loudness * jnp.repeat(steps, extent[axis_at] // blocks).reshape([-1 if axis == axis_at else 1 for axis in range(len(extent))])
    return loudness


def rank_bounds(amount, skew):
    loads = [(1 << 20) // math.isqrt(rank ** skew) + 1 for rank in range(1, amount + 1)]
    width = 1 + sum(loads) // (1 << 30)
    return np.cumsum(np.array([max(1, weight // width) for weight in loads]))


def ranked(stream_key, extent, amount, skew):
    listing = rank_bounds(amount, skew)
    ticket = jax.random.randint(jax.random.fold_in(stream_key, 1), extent, 0, int(listing[amount - 1]))
    standing = jnp.searchsorted(jnp.asarray(listing, jnp.int32), ticket, side="right")
    return jax.random.permutation(jax.random.fold_in(stream_key, 2), amount)[standing].astype(jnp.int32)


def scatter_about(key, dims, deviation, most, split=(), held_as=jnp.bfloat16):
    entries = jax.random.normal(key, dims, jnp.float32) * deviation
    if len(split) > 0:
        entries = block_levels(key, dims, split, -0.22, 0.18) * entries
    return jnp.clip(entries, min=-most, max=most).astype(held_as)


def setup_inputs(seed: int = 0) -> dict:
    streams_of = jax.random.split(jax.random.key(seed), 7)
    pool_old = jnp.clip(0.5 + 1.5 * jax.random.uniform(streams_of[0], (POOLS, PATCHES), jnp.float32) ** block_levels(streams_of[0], (POOLS, PATCHES), ((1, 32),), -0.2, 0.2), 0.5, 2.0)
    pool_new = jnp.clip(0.5 + 1.5 * jax.random.uniform(streams_of[1], (POOLS, PATCHES), jnp.float32) ** block_levels(streams_of[1], (POOLS, PATCHES), ((1, 32),), -0.2, 0.2), 0.5, 2.0)
    flux = scatter_about(streams_of[2], (POOLS, PATCHES), 1.0, 6.0, ((1, 32),), jnp.float32)
    area = jnp.clip(jnp.exp(math.log(1.0) - 2.9957323 * jax.random.uniform(streams_of[3], (PATCHES,), jnp.float32) ** block_levels(streams_of[3], (PATCHES,), ((0, 32),), -0.2, 0.2)), 0.05, 1.0)
    pft_id = plant(ranked(streams_of[4], (PATCHES,), PFT, 2), jax.random.fold_in(streams_of[4], 3), 0, PFT - 1).astype(jnp.int32)
    region_id = draw_region_id(jax.random.fold_in(streams_of[6], 71), 0)
    return {"pool_old": pool_old, "pool_new": pool_new, "flux": flux, "area": area, "pft_id": pft_id, "region_id": region_id}


def reference(pool_old, pool_new, flux, area, pft_id, region_id):
    cell = (pft_id * REGION + region_id).astype(jnp.int32)
    stored = area[None, :] * pool_new
    balance = area[None, :] * (pool_new - pool_old - 0.5 * flux)
    stacked = jnp.concatenate([stored, balance], axis=0)
    totals = jax.ops.segment_sum(stacked.T, cell, num_segments=CELLS).T
    totals = totals * jnp.float32(CELLS / PATCHES)
    return (totals[:POOLS], totals[POOLS:])
```

```python
import functools

import jax
import jax.numpy as jnp
from jax import lax
from jax.experimental import pallas as pl
from jax.experimental.pallas import tpu as pltpu
from jax.sharding import PartitionSpec as P

POOLS = 40
PFT = 79
REGION = 32
CELLS = 2528
GROUP = 28
GROUPS = 3
ROWS = 2 * GROUP
LANES = 128
AXES = ("gx", "gy")


def table_kernel(scale, base_ref, old_ref, new_ref, flux_ref, area_ref, pft_ref, region_ref, out_ref, acc_ref):
    step = pl.program_id(0)

    @pl.when(step == 0)
    def _():
        acc_ref[...] = jnp.zeros_like(acc_ref)

    area = area_ref[...]
    new = new_ref[...]
    stored = area * new
    balance = area * (new - old_ref[...] - 0.5 * flux_ref[...])
    values = jnp.concatenate([stored, balance], axis=0)
    high = values.astype(jnp.bfloat16)
    rest = values - high.astype(jnp.float32)
    middle = rest.astype(jnp.bfloat16)
    low = (rest - middle.astype(jnp.float32)).astype(jnp.bfloat16)
    parts = jnp.concatenate([high, middle, low], axis=0)
    pft = pft_ref[...]
    group = (pft >= GROUP).astype(jnp.int32) + (pft >= 2 * GROUP).astype(jnp.int32)
    here = (region_ref[...] != base_ref[0]).astype(jnp.int32)
    cell = here * 96 + group * (32 - GROUP) + pft
    rows = lax.broadcasted_iota(jnp.int32, (192, cell.shape[1]), 0)
    onehot = (rows == cell).astype(jnp.bfloat16)
    acc_ref[...] += lax.dot_general(
        onehot, parts, (((1,), (1,)), ((), ())), preferred_element_type=jnp.float32
    )

    @pl.when(step == pl.num_programs(0) - 1)
    def _():
        both = 2 * POOLS
        total = acc_ref[...]
        total = (total[:, :both] + total[:, both : 2 * both] + total[:, 2 * both : 3 * both]) * scale
        for j in range(2):
            for s in range(2):
                pieces = [
                    total[j * 96 + g * 32 : j * 96 + g * 32 + GROUP, s * POOLS : (s + 1) * POOLS]
                    for g in range(GROUPS)
                ]
                pieces.append(jnp.zeros((GROUP, LANES - GROUPS * POOLS), jnp.float32))
                out_ref[j, s * GROUP : (s + 1) * GROUP, :] = jnp.concatenate(pieces, axis=1)


def local_tables(scale, base, pool_old, pool_new, flux, area, pft_id, region_id):
    patches = area.shape[0]
    chunk = min(1024, patches)
    wide = pl.BlockSpec((POOLS, chunk), lambda k: (0, k))
    narrow = pl.BlockSpec((1, chunk), lambda k: (0, k))
    return pl.pallas_call(
        functools.partial(table_kernel, scale),
        grid=(patches // chunk,),
        out_shape=jax.ShapeDtypeStruct((2, ROWS, LANES), jnp.float32),
        in_specs=[pl.BlockSpec(memory_space=pltpu.SMEM), wide, wide, wide, narrow, narrow, narrow],
        out_specs=pl.BlockSpec((2, ROWS, LANES), lambda k: (0, 0, 0)),
        scratch_shapes=[pltpu.VMEM((192, 240), jnp.float32)],
        name="local_tables",
    )(
        base.reshape(1),
        pool_old,
        pool_new,
        flux,
        area.reshape(1, patches),
        pft_id.reshape(1, patches),
        region_id.reshape(1, patches),
    )


def assemble_kernel(table_ref, stored_ref, balance_ref):
    for s, out_ref in enumerate((stored_ref, balance_ref)):
        for quad in range(GROUP // 4):
            block = jnp.concatenate(
                [table_ref[pl.ds(s * GROUP + quad * 4 + i, REGION, stride=ROWS), :] for i in range(4)],
                axis=0,
            ).T
            for g in range(GROUPS):
                column = (g * (GROUP // 4) + quad) * LANES
                width = min(LANES, CELLS - column)
                if width > 0:
                    out_ref[:, column : column + width] = block[g * POOLS : (g + 1) * POOLS, :width]


def assemble(tables):
    return pl.pallas_call(
        assemble_kernel,
        out_shape=[jax.ShapeDtypeStruct((POOLS, CELLS), jnp.float32)] * 2,
        name="assemble",
    )(tables.reshape(REGION * ROWS, LANES))


def join(low, high, axis):
    count = low.shape[axis]
    cut = lambda table, first, last: lax.slice_in_dim(table, first, last, axis=axis)
    return jnp.concatenate(
        [cut(low, 0, count - 1), cut(low, count - 1, count) + cut(high, 0, 1), cut(high, 1, count)],
        axis=axis,
    )


def gather_regions(tables, position, width_x, width_y):
    devices = width_x * width_y

    def exchange(mine, step):
        other = lax.ppermute(mine, AXES, [(i, i ^ step) for i in range(devices)])
        lower = (position // step) % 2 == 0
        return jnp.where(lower, mine, other), jnp.where(lower, other, mine)

    step = 1
    while step < width_y:
        tables = join(*exchange(tables, step), 0)
        step *= 2
    tables = tables[None]
    step = devices // 2
    while step >= width_y:
        tables = jnp.stack(exchange(tables, step), axis=1)
        tables = tables.reshape(-1, *tables.shape[2:])
        step //= 2
    while tables.shape[0] > 1:
        tables = join(tables[0::2], tables[1::2], 1)
    tables = tables[0]
    return jnp.concatenate([tables[:1] + tables[-1:], tables[1:-1]], axis=0)


def shards(pool_old, pool_new, flux, area, pft_id, region_id):
    width_x = lax.axis_size("gx")
    width_y = lax.axis_size("gy")
    devices = width_x * width_y
    position = lax.axis_index("gx") * width_y + lax.axis_index("gy")
    base = position * REGION // devices
    scale = CELLS / (area.shape[0] * devices)
    tables = local_tables(scale, base, pool_old, pool_new, flux, area, pft_id, region_id)
    if devices == REGION and width_x & (width_x - 1) == 0:
        tables = gather_regions(tables, position, width_x, width_y)
    else:
        here = (base + jnp.arange(2, dtype=jnp.int32)) % REGION
        spread = jnp.zeros((REGION, ROWS, LANES), jnp.float32).at[here].add(tables)
        tables = lax.psum(lax.psum(spread, "gy"), "gx")
    return tuple(assemble(tables))


def solution(mesh):
    return jax.shard_map(
        shards,
        mesh=mesh,
        in_specs=(
            P(None, ("gx", "gy")),
            P(None, ("gx", "gy")),
            P(None, ("gx", "gy")),
            P(("gx", "gy")),
            P(("gx", "gy")),
            P(("gx", "gy")),
        ),
        out_specs=(P(), P()),
        check_vma=False,
    )
```

```python
import functools

import jax
import jax.numpy as jnp
from jax import lax
from jax.experimental import pallas as pl
from jax.experimental.pallas import tpu as pltpu
from jax.sharding import PartitionSpec as P

POOLS = 40
PFT = 79
REGION = 32
CELLS = 2528
GROUP = 28
GROUPS = 3
ROWS = 2 * GROUP
LANES = 128
HALVES = (32, 24)
SLOT = 32
PAIR = GROUPS * SLOT
AXES = ("gx", "gy")
MIB = 1 << 20


def table_kernel(
    scale, chunk, old_hbm, new_hbm, flux_hbm, area_hbm, pft_hbm, region_hbm,
    first_ref, second_ref, old_ref, new_ref, flux_ref, area_ref, pft_ref, region_ref, acc_ref, sems,
):
    patches = area_hbm.shape[1]
    width_y = lax.axis_size("gy")
    devices = lax.axis_size("gx") * width_y
    base = (lax.axis_index("gx") * width_y + lax.axis_index("gy")) * REGION // devices
    pairs = (
        (pft_hbm, pft_ref), (region_hbm, region_ref), (area_hbm, area_ref),
        (new_hbm, new_ref), (old_hbm, old_ref), (flux_hbm, flux_ref),
    )
    copies = []
    for k in range(patches // chunk):
        part = pl.ds(k * chunk, chunk)
        copies.append(
            [pltpu.make_async_copy(a.at[:, part], b.at[:, part], sems.at[n, k]) for n, (a, b) in enumerate(pairs)]
        )
        for copy in copies[-1]:
            copy.start()
    for k, started in enumerate(copies):
        part = pl.ds(k * chunk, chunk)
        for copy in started:
            copy.wait()
        pft = pft_ref[:, part]
        group = (pft >= GROUP).astype(jnp.int32) + (pft >= 2 * GROUP).astype(jnp.int32)
        here = (region_ref[:, part] != base).astype(jnp.int32)
        cell = here * PAIR + group * (SLOT - GROUP) + pft
        columns = lax.broadcasted_iota(jnp.int32, (2 * PAIR, chunk), 0)
        onehot = (columns == cell).astype(jnp.bfloat16)
        area = area_ref[:, part]
        new = new_ref[:, part]
        stored = area * new
        balance = area * (new - old_ref[:, part] - 0.5 * flux_ref[:, part])
        values = jnp.concatenate([stored, balance], axis=0)
        high = values.astype(jnp.bfloat16)
        rest = values - high.astype(jnp.float32)
        middle = rest.astype(jnp.bfloat16)
        low = (rest - middle.astype(jnp.float32)).astype(jnp.bfloat16)
        parts = jnp.concatenate([high, middle, low], axis=0)
        added = lax.dot_general(
            parts, onehot, (((1,), (1,)), ((), ())), preferred_element_type=jnp.float32
        )
        if k == 0:
            acc_ref[...] = added
        else:
            acc_ref[...] += added
    both = 2 * POOLS
    total = acc_ref[...]
    total = (total[:both] + total[both : 2 * both] + total[2 * both :]) * scale
    total = jnp.concatenate([total, jnp.zeros((LANES - both, 2 * PAIR), jnp.float32)], axis=0).T
    for j in range(2):
        table = []
        for s in range(2):
            pieces = [
                total[j * PAIR + g * SLOT : j * PAIR + g * SLOT + GROUP, s * POOLS : (s + 1) * POOLS]
                for g in range(GROUPS)
            ]
            pieces.append(jnp.zeros((GROUP, LANES - GROUPS * POOLS), jnp.float32))
            table.append(jnp.concatenate(pieces, axis=1))
        table = jnp.concatenate(table, axis=0)
        first_ref[j] = table[: HALVES[0]]
        second_ref[j] = table[HALVES[0] :]


def local_tables(scale, pool_old, pool_new, flux, area, pft_id, region_id):
    patches = area.shape[0]
    chunk = min(1024, patches)
    steps = patches // chunk
    wide = pltpu.VMEM((POOLS, patches), jnp.float32)
    return pl.pallas_call(
        functools.partial(table_kernel, scale, chunk),
        out_shape=[jax.ShapeDtypeStruct((2, rows, LANES), jnp.float32) for rows in HALVES],
        in_specs=[pl.BlockSpec(memory_space=pltpu.HBM)] * 6,
        out_specs=[pl.BlockSpec(memory_space=pltpu.VMEM)] * 2,
        scratch_shapes=[
            wide,
            wide,
            wide,
            pltpu.VMEM((1, patches), jnp.float32),
            pltpu.VMEM((1, patches), jnp.int32),
            pltpu.VMEM((1, patches), jnp.int32),
            pltpu.VMEM((6 * POOLS, 2 * PAIR), jnp.float32),
            pltpu.SemaphoreType.DMA((6, steps)),
        ],
        compiler_params=pltpu.CompilerParams(vmem_limit_bytes=16 * MIB),
        name="local_tables",
    )(
        *(
            pltpu.with_memory_space_constraint(operand, pltpu.HBM)
            for operand in (
                pool_old,
                pool_new,
                flux,
                area.reshape(1, patches),
                pft_id.reshape(1, patches),
                region_id.reshape(1, patches),
            )
        )
    )


def assemble_kernel(masks, span, half_rows, sources, *refs):
    count = len(masks)
    out_ref = refs[count * len(half_rows)]
    full_refs = refs[count * len(half_rows) + 1 :]
    me = lax.axis_index("gx") if count > 1 else 0
    for h, rows in enumerate(half_rows):
        full_ref = full_refs[h]
        for m, mask in enumerate(masks):
            full_ref[me ^ mask] = refs[h * count + m][...].reshape((span + 1) * rows, LANES)
        for r in range(count):
            full_ref[r, :rows] += full_ref[(r - 1) % count, span * rows :]
    for quad in range(GROUP // 4):
        block = []
        for i in range(4):
            h, row = sources[quad * 4 + i]
            rows = half_rows[h]
            block += [full_refs[h][r, pl.ds(row, span, stride=rows), :] for r in range(count)]
        block = jnp.concatenate(block, axis=0).T
        for g in range(GROUPS):
            column = (g * (GROUP // 4) + quad) * LANES
            width = min(LANES, CELLS - column)
            if width > 0:
                out_ref[:, column : column + width] = block[g * POOLS : (g + 1) * POOLS, :width]


def assemble(name, masks, halves, sources):
    half_rows = [pieces[0].shape[1] for pieces in halves]
    span = halves[0][0].shape[0] - 1
    pieces = [piece for half in halves for piece in half]
    return pl.pallas_call(
        functools.partial(assemble_kernel, masks, span, half_rows, sources),
        out_shape=jax.ShapeDtypeStruct((POOLS, CELLS), jnp.float32),
        in_specs=[pl.BlockSpec(memory_space=pltpu.VMEM)] * len(pieces),
        out_specs=pl.BlockSpec(memory_space=pltpu.VMEM),
        scratch_shapes=[
            pltpu.VMEM((len(masks), (span + 1) * rows, LANES), jnp.float32) for rows in half_rows
        ],
        compiler_params=pltpu.CompilerParams(vmem_limit_bytes=8 * MIB),
        name=name,
    )(*pieces)


def join(low, high):
    return jnp.concatenate([low[:-1], low[-1:] + high[:1], high[1:]], axis=0)


def gather_rows(halves, position, width_x, width_y):
    devices = width_x * width_y

    def send(mine, step):
        return lax.ppermute(mine, AXES, [(i, i ^ step) for i in range(devices)])

    step = 1
    while step < width_y:
        lower = (position // step) % 2 == 0
        others = [send(mine, step) for mine in halves]
        halves = [
            join(jnp.where(lower, mine, other), jnp.where(lower, other, mine))
            for mine, other in zip(halves, others)
        ]
        step *= 2
    masks = [0]
    halves = [[mine] for mine in halves]
    mask = width_x // 2
    while mask:
        masks = masks + [m ^ mask for m in masks]
        halves = [pieces + [send(piece, mask * width_y) for piece in pieces] for pieces in halves]
        mask //= 2
    return masks, halves


def shards(pool_old, pool_new, flux, area, pft_id, region_id):
    width_x = lax.axis_size("gx")
    width_y = lax.axis_size("gy")
    devices = width_x * width_y
    position = lax.axis_index("gx") * width_y + lax.axis_index("gy")
    scale = CELLS / (area.shape[0] * devices)
    halves = local_tables(scale, pool_old, pool_new, flux, area, pft_id, region_id)
    if devices == REGION and width_x & (width_x - 1) == 0:
        masks, halves = gather_rows(halves, position, width_x, width_y)
    else:
        here = (position * REGION // devices + jnp.arange(2, dtype=jnp.int32)) % REGION
        full = []
        for tables in halves:
            spread = jnp.zeros((REGION + 1, *tables.shape[1:]), jnp.float32).at[here].add(tables)
            full.append([lax.psum(lax.psum(spread, "gy"), "gx")])
        masks, halves = [0], full
    first = HALVES[0]
    stored = assemble("stored", masks, halves[:1], [(0, i) for i in range(GROUP)])
    balance = assemble(
        "balance",
        masks,
        halves,
        [(0, i) if i < first else (1, i - first) for i in range(GROUP, 2 * GROUP)],
    )
    return stored, balance


def solution(mesh):
    return jax.shard_map(
        shards,
        mesh=mesh,
        in_specs=(
            P(None, ("gx", "gy")),
            P(None, ("gx", "gy")),
            P(None, ("gx", "gy")),
            P(("gx", "gy")),
            P(("gx", "gy")),
            P(("gx", "gy")),
        ),
        out_specs=(P(), P()),
        check_vma=False,
    )
```
